768 devices in a mesh: grp: 96 (over x, z, core), sub: 8 (over y).
Axes of the slice: x: 4, y: 8, z: 12, core: 2. Of those that a mesh axis runs over, the one named last changes fastest.
Arguments:
- child_moments: bfloat16 [294, 786432], P(None, ('grp', 'sub')), may hold values from -6 to 6
- upward_matrix: bfloat16 [294, 8, 294], replicated, may hold values from -0.125 to 0.125
- project_matrix: bfloat16 [64, 294], replicated, may hold values from -0.375 to 0.375
- transfer_matrix: bfloat16 [64, 20224], replicated, may hold values from -0.0546875 to 0.0546875
- expand_matrix: bfloat16 [294, 64], replicated, may hold values from -0.75 to 0.75
- downward_matrix: bfloat16 [294, 8, 294], replicated, may hold values from -0.375 to 0.375
- neighbour_list: int32 [316, 98304], P(None, ('grp', 'sub')), may hold values from 0 to 8704, as said below
- ghost_map: int32 [768, 960], P(('grp', 'sub')), may hold values from 0 to 128, as said below
Outputs:
- child_locals: bfloat16 [294, 786432], P(None, ('grp', 'sub'))
The draws below stay inside these ranges and needn't reach their ends.
Inputs may be any that keep to these rules, and one draw needn't show every extreme that they name: `neighbour_list`: entries below 8704 name a source slot; each column has between 95 and 189 such entries, and the first column of every device's block has exactly 189. Every ghost slot that is named holds a box. `ghost_map`: the groups stand in a three-dimensional arrangement; a device sends boxes only to groups next to its own there (all other destinations hold 128 only). Slot 0 of every such destination names a box, and every device fills all 10 slots of at least one destination.
All inputs are finite; a program needn't handle non-finite values.
Results may differ from the reference program's by a relative error of at most 0.0085.
Values may be sent and summed in bfloat16 or wider, within the bound.
A program may use at most 64 MiB of HBM per device.

```python
import jax
import jax.numpy as jnp
from jax import lax

NE = 98
RANK = 64
OFFS = 316
VLIST = 189
GHOST = 10
BOX_DEV = 128
SENDERS = 768
TARGETS = 98304
CHILDREN = 786432
GROUP_SLOTS = 960
POOL = 8704
N_GRP = 96
N_SUB = 8


def group_shape():
    half = N_GRP // 2
    rows = 1
    for cand in range(1, half + 1):
        if half % cand == 0 and cand * cand <= half:
            rows = cand
    return (half, half // rows)


def ghost_table(key):
    half, cols = group_shape()
    groups = jnp.arange(N_GRP, dtype=jnp.int32)
    layer = groups // half
    row_pos = groups % half // cols
    col_pos = groups % cols
    near = (jnp.abs(layer[:, None] - layer[None, :]) <= 1) & (jnp.abs(row_pos[:, None] - row_pos[None, :]) <= 1)
    near = near & (jnp.abs(col_pos[:, None] - col_pos[None, :]) <= 1) & (groups[:, None] != groups[None, :])
    sender_group = jnp.arange(SENDERS, dtype=jnp.int32) // N_SUB
    near_send = near[sender_group]
    partner = (sender_group + half) % N_GRP
    count = jax.random.randint(jax.random.fold_in(key, 31), (SENDERS, N_GRP), 1, GHOST + 1)
    count = jnp.where(groups[None, :] == partner[:, None], GHOST, count)
    box_ids = jax.random.randint(jax.random.fold_in(key, 32), (SENDERS, N_GRP, GHOST), 0, BOX_DEV)
    slot_index = jnp.arange(GHOST, dtype=jnp.int32).reshape(1, 1, GHOST)
    live = near_send[:, :, None] & (slot_index < count[:, :, None])
    return jnp.where(live, box_ids, BOX_DEV).astype(jnp.int32)


def draw_ghost_map(key, part):
    return ghost_table(key).reshape(SENDERS, GROUP_SLOTS).astype(jnp.int32)


def draw_neighbour_list(key, part):
    group_boxes = N_SUB * BOX_DEV
    ghost_total = N_SUB * N_GRP * GHOST
    table = ghost_table(key).reshape(N_GRP, N_SUB, N_GRP, GHOST)
    live = jnp.transpose(table, (2, 1, 0, 3)).reshape(N_GRP, ghost_total) < BOX_DEV
    ranks = jnp.where(live, 0, 1) * ghost_total + jnp.arange(ghost_total, dtype=jnp.int32)[None, :]
    order = jnp.argsort(ranks, axis=1).astype(jnp.int32)
    live_total = jnp.sum(live.astype(jnp.int32), axis=1)
    target_group = jnp.arange(TARGETS, dtype=jnp.int32) // group_boxes
    bits = jax.random.randint(jax.random.fold_in(key, 24), (OFFS, TARGETS), 0, 1 << 20)
    pick = bits % live_total[target_group][None, :]
    ghost_col = order[target_group[None, :], pick] + group_boxes
    own_col = jax.random.randint(jax.random.fold_in(key, 25), (OFFS, TARGETS), 0, group_boxes)
    use_own = jax.random.randint(jax.random.fold_in(key, 26), (OFFS, TARGETS), 0, 2) == 1
    source = jnp.where(use_own, own_col, ghost_col)
    live_count = VLIST - jax.random.randint(jax.random.fold_in(key, 21), (TARGETS,), 0, VLIST // 2 + 1)
    first_box = jnp.arange(TARGETS) % BOX_DEV == 0
    live_count = jnp.where(first_box, VLIST, live_count)
    scores = jax.random.randint(jax.random.fold_in(key, 22), (OFFS, TARGETS), 0, 1 << 20) * OFFS + jnp.arange(OFFS).reshape(OFFS, 1)
    ranking = jnp.argsort(scores, axis=0)
    position = jnp.argsort(ranking, axis=0)
    return jnp.where(position < live_count[None, :], source, POOL).astype(jnp.int32)


def steps_of(key, extent, shards, low, high):
    gain, own = 1.0, jax.random.fold_in(key, 6)
    for axis_at, blocks in shards:
        steps = jnp.exp(jax.random.uniform(jax.random.fold_in(own, axis_at), (blocks,), jnp.float32, low / len(shards), high / len(shards)))
        gain = gain * jnp.repeat(steps, extent[axis_at] // blocks).reshape([-1 if axis == axis_at else 1 for axis in range(len(extent))])
    return gain


def noise(rng, shape, scale, most, pieces=(), held_as=jnp.bfloat16):
    values = scale * jax.random.normal(rng, shape, jnp.float32)
    if pieces:
        values = values * steps_of(rng, shape, pieces, -0.22, 0.18)
    return jnp.clip(values, -most, most).astype(held_as)


def setup_inputs(seed: int = 0) -> dict:
    splits = jax.random.split(jax.random.key(seed), 9)
    child_moments = noise(splits[0], (3 * NE, CHILDREN), 1.0, 6.0, ((1, 768),))
    upward_matrix = noise(splits[1], (3 * NE, 8, 3 * NE), (24 * NE) ** -0.5, 0.125)
    project_matrix = noise(splits[2], (RANK, 3 * NE), (3 * NE) ** -0.5, 0.375)
    transfer_matrix = noise(splits[3], (RANK, OFFS * RANK), (VLIST * RANK) ** -0.5, 0.0546875)
    expand_matrix = noise(splits[4], (3 * NE, RANK), RANK ** -0.5, 0.75)
    downward_matrix = noise(splits[5], (3 * NE, 8, 3 * NE), (3 * NE) ** -0.5, 0.375)
    neighbour_list = draw_neighbour_list(jax.random.fold_in(splits[8], 71), 0)
    ghost_map = draw_ghost_map(jax.random.fold_in(splits[8], 71), 0)
    return {"child_moments": child_moments, "upward_matrix": upward_matrix, "project_matrix": project_matrix, "transfer_matrix": transfer_matrix, "expand_matrix": expand_matrix, "downward_matrix": downward_matrix, "neighbour_list": neighbour_list, "ghost_map": ghost_map}


def reference(child_moments, upward_matrix, project_matrix, transfer_matrix, expand_matrix, downward_matrix, neighbour_list, ghost_map):
    surface = 3 * NE
    group_boxes = N_SUB * BOX_DEV
    upward_float = upward_matrix.astype(jnp.float32)
    downward_float = downward_matrix.astype(jnp.float32)
    children = jnp.moveaxis(child_moments.reshape(surface, N_GRP, N_SUB, 8, BOX_DEV), 1, 0)

    def upward(group_block):
        parent = jnp.einsum("icj,jscb->isb", upward_float, group_block.astype(jnp.float32)).astype(jnp.bfloat16)
        return jnp.dot(project_matrix, parent.reshape(surface, group_boxes), preferred_element_type=jnp.float32).astype(jnp.bfloat16)

    packed = lax.map(upward, children)
    flat_packed = jnp.moveaxis(packed, 0, 1).reshape(RANK, TARGETS)
    padded = jnp.concatenate([flat_packed, jnp.zeros((RANK, 1), jnp.bfloat16)], axis=1)
    send_table = ghost_map.reshape(N_GRP, N_SUB, N_GRP, GHOST)
    device_base = (jnp.arange(N_GRP * N_SUB, dtype=jnp.int32) * BOX_DEV).reshape(N_GRP, N_SUB, 1, 1)
    ghost_column = jnp.where(send_table < BOX_DEV, device_base + send_table, TARGETS).astype(jnp.int32)
    ghost_column = jnp.transpose(ghost_column, (2, 1, 0, 3)).reshape(N_GRP, N_SUB * N_GRP * GHOST)
    neighbours = jnp.moveaxis(neighbour_list.reshape(OFFS, N_GRP, group_boxes), 1, 0)
    translate = transfer_matrix.astype(jnp.float32).reshape(RANK, OFFS, RANK)

    def downward(inputs):
        own_packed, columns, lists = inputs
        source_pool = jnp.concatenate([own_packed, padded[:, columns], jnp.zeros((RANK, 1), jnp.bfloat16)], axis=1)
        picked = source_pool[:, lists].astype(jnp.float32)
        local_coeff = jnp.einsum("roq,qot->rt", translate, picked).astype(jnp.bfloat16)
        local_moment = jnp.dot(expand_matrix, local_coeff, preferred_element_type=jnp.float32).astype(jnp.bfloat16)
        moment_float = local_moment.astype(jnp.float32).reshape(surface, N_SUB, BOX_DEV)
        return jnp.einsum("icj,jsb->iscb", downward_float, moment_float).astype(jnp.bfloat16)

    result = lax.map(downward, (packed, ghost_column, neighbours))
    return jnp.moveaxis(result, 0, 1).reshape(surface, CHILDREN)
```

```python
import functools
import jax
import jax.numpy as jnp
from jax import lax
from jax.experimental import pallas as pl
from jax.experimental.pallas import tpu as pltpu
from jax.sharding import PartitionSpec as P

F32=jnp.float32; BF=jnp.bfloat16
NT=(((1,),(1,)),((),()))
def kb(idx_ref, pool_ref, t_ref, e_ref, d_ref, out_ref, taba, tabb, st0, st1, dsc, acc):
    n = pool_ref.shape[0]
    ch = 256
    zero64 = jnp.zeros((ch,64),F32)
    @pl.loop(0, n//ch)
    def _(r):
        rows = pl.ds(pl.multiple_of(r*ch,ch),ch)
        x = pool_ref[rows,:].astype(F32)
        taba[rows,:] = jnp.concatenate([x,zero64],axis=1)
        tabb[rows,:] = jnp.concatenate([zero64,x],axis=1)
    taba[pl.ds(n,8),:] = jnp.zeros((8,128),F32)
    tabb[pl.ds(n,8),:] = jnp.zeros((8,128),F32)
    acc[...] = jnp.zeros_like(acc)
    pairs = idx_ref.shape[0]//4
    def gather(kk, st):
        for j in range(2):
            o = 4*kk+2*j
            for t in range(128):
                st[j, pl.ds(t,1), :] = taba[pl.ds(idx_ref[o,t],1),:] + tabb[pl.ds(idx_ref[o+1,t],1),:]
    @pl.loop(0, pairs)
    def _(kk):
        gather(kk, st0)
        p = jnp.concatenate([st0[0],st0[1]],axis=1).astype(BF)
        tt = t_ref[:, pl.ds(pl.multiple_of(kk*256,256),256)]
        acc[...] += lax.dot_general(tt, p, NT, preferred_element_type=F32)
    lc = acc[...].astype(BF)
    lm = jnp.dot(e_ref[...], lc, preferred_element_type=F32).astype(BF)
    ne = d_ref.shape[0]
    d2 = d_ref[...].reshape(ne*8, ne)
    dsc[...] = jnp.dot(d2, lm, preferred_element_type=F32)
    for c in range(8):
        out_ref[:, c*128:(c+1)*128] = dsc[pl.ds(c, ne, stride=8),:].astype(BF)

def m2l(idx, pool, t, e, d):
    ne = d.shape[0]
    n = pool.shape[0]
    V=pl.BlockSpec(memory_space=pltpu.VMEM)
    return pl.pallas_call(kb, out_shape=jax.ShapeDtypeStruct((ne,1024),BF),
      in_specs=[pl.BlockSpec(memory_space=pltpu.SMEM),V,V,V,V], out_specs=V,
      scratch_shapes=[pltpu.VMEM((n+8,128),F32),pltpu.VMEM((n+8,128),F32),pltpu.VMEM((2,128,128),F32),pltpu.VMEM((2,128,128),F32),pltpu.VMEM((ne*8,128),F32),pltpu.VMEM((64,128),F32)],
      compiler_params=pltpu.CompilerParams(vmem_limit_bytes=56*2**20))(idx,pool,t,e,d)
def in_order(pieces, dim):
    pieces = jnp.moveaxis(pieces, 0, dim)
    shape = pieces.shape
    return pieces.reshape(*shape[:dim], shape[dim] * shape[dim + 1], *shape[dim + 2 :])


def from_everyone(x, axis):
    copies = jnp.broadcast_to(x, (lax.axis_size(axis), *x.shape))
    return lax.all_to_all(copies, axis, split_axis=0, concat_axis=0, tiled=True)


def gather_directly(x, axis, dim):
    return in_order(from_everyone(x, axis), dim)


def on_device(
    child_moments,
    upward_matrix,
    project_matrix,
    transfer_matrix,
    expand_matrix,
    downward_matrix,
    neighbour_list,
    ghost_map,
):
    surface = child_moments.shape[0]
    box_count = child_moments.shape[1] // 8
    coeff_rows = project_matrix.shape[0]
    children = child_moments.reshape(surface, 8, box_count)
    parent = jnp.einsum(
        "icj,jcb->ib", upward_matrix, children, preferred_element_type=jnp.float32
    ).astype(jnp.bfloat16)
    packed_rows = lax.dot_general(
        parent, project_matrix, (((0,), (1,)), ((), ())), preferred_element_type=jnp.float32
    ).astype(jnp.bfloat16)
    slot_ids = ghost_map.reshape(-1)
    source = jnp.concatenate([packed_rows, jnp.zeros((1, coeff_rows), jnp.bfloat16)], axis=0)[
        slot_ids
    ]
    ghosts = lax.all_to_all(source, "grp", split_axis=0, concat_axis=0, tiled=True)
    mine = jnp.concatenate([packed_rows, ghosts], axis=0)
    sub_count = lax.axis_size("sub")
    ghost_width = ghosts.shape[0]
    width = box_count + ghost_width
    group_boxes = sub_count * box_count
    pool_size = sub_count * width
    lists = neighbour_list
    ghost_index = lists - group_boxes
    own_place = lists // box_count * width + lists % box_count
    ghost_place = ghost_index // ghost_width * width + box_count + ghost_index % ghost_width
    remap = jnp.where(lists < group_boxes, own_place, ghost_place)
    remap = jnp.where(lists < pool_size, remap, pool_size)
    whole_pool = gather_directly(mine, "sub", 0)
    return m2l(remap, whole_pool, transfer_matrix, expand_matrix, downward_matrix)


def solution(mesh):
    return jax.shard_map(
        on_device,
        mesh=mesh,
        in_specs=(
            P(None, ("grp", "sub")),
            P(),
            P(),
            P(),
            P(),
            P(),
            P(None, ("grp", "sub")),
            P(("grp", "sub"), None),
        ),
        out_specs=P(None, ("grp", "sub")),
        check_vma=False,
    )
```

```python
import functools
import jax
import jax.numpy as jnp
from jax import lax
from jax.experimental import pallas as pl
from jax.experimental.pallas import tpu as pltpu

from jax.sharding import PartitionSpec as P

F32, BF, I32 = jnp.float32, jnp.bfloat16, jnp.int32
NT = (((1,), (1,)), ((), ()))
VM = pl.BlockSpec(memory_space=pltpu.VMEM)
GH_ROWS = 144


def exchange_kernel(n_grp, n_sub, gs_ref, gv_ref, x_ref, u_ref, p_ref, own_out, gh_out, rank_out,
                    uf, tab, sf, send, recv, own, ownr, comp, ghr, hot,
                    own_send, own_recv, slot_send, slot_recv, gh_send, gh_recv):
    me_g, me_s = lax.axis_index("grp"), lax.axis_index("sub")
    ne = u_ref.shape[0]
    barrier = pltpu.get_barrier_semaphore()

    def grp_peer(d):
        return lax.rem(me_g + d, n_grp)

    def sub_peer(d):
        return lax.rem(me_s + d, n_sub)

    @pl.loop(1, n_grp)
    def _(d):
        pl.semaphore_signal(barrier, inc=1, device_id={"grp": grp_peer(d), "sub": me_s},
                            device_id_type=pl.DeviceIdType.MESH)

    @pl.loop(1, n_sub)
    def _(d):
        pl.semaphore_signal(barrier, inc=1, device_id={"grp": me_g, "sub": sub_peer(d)},
                            device_id_type=pl.DeviceIdType.MESH)

    flat = u_ref[...].reshape(ne * 8, ne).astype(F32)
    starts = range(0, ne, 128)
    for n, at in enumerate(starts):
        width = min(128, ne - at)
        uf[n, :, pl.ds(0, width)] = flat[:, at : at + width]
    total = jnp.zeros((ne, 128), F32)
    for c in range(8):
        tiles = [uf[n, pl.ds(c, ne, stride=8), :].astype(BF) for n in range(len(starts))]
        tiles[-1] = tiles[-1][:, : ne - starts[-1]]
        total += jnp.dot(jnp.concatenate(tiles, axis=1), x_ref[:, c * 128 : (c + 1) * 128],
                         preferred_element_type=F32)
    parent = total.astype(BF)
    twice = jnp.concatenate([p_ref[...], p_ref[...]], axis=0)
    packed = jnp.dot(twice, parent, preferred_element_type=F32).T.astype(BF).astype(F32)
    lo64 = lax.broadcasted_iota(I32, (1, 128), 1) < 64
    tab[pl.ds(0, 128), :] = packed
    tab[pl.ds(128, 8), :] = jnp.zeros((8, 128), F32)
    mine = jnp.where(lo64, packed[0:64], packed[64:128]).astype(BF)
    own[...] = mine
    ownr[me_s] = mine
    sf[...] = jnp.zeros_like(sf)

    @pl.loop(0, n_grp)
    def _(g):
        for k in range(5):
            sf[g, pl.ds(k, 1), :] = jnp.where(lo64, tab[pl.ds(gs_ref[0, g * 10 + k], 1), :],
                                              tab[pl.ds(gs_ref[0, g * 10 + 5 + k], 1), :])

    send[...] = sf[...].astype(BF)
    recv[me_g] = send[me_g]
    pl.semaphore_wait(barrier, n_grp + n_sub - 2)

    def own_copy(d):
        return pltpu.make_async_remote_copy(
            src_ref=own, dst_ref=ownr.at[me_s], send_sem=own_send, recv_sem=own_recv,
            device_id={"grp": me_g, "sub": sub_peer(d)}, device_id_type=pl.DeviceIdType.MESH)

    def slot_copy(d):
        g = grp_peer(d)
        return pltpu.make_async_remote_copy(
            src_ref=send.at[g], dst_ref=recv.at[me_g], send_sem=slot_send, recv_sem=slot_recv,
            device_id={"grp": g, "sub": me_s}, device_id_type=pl.DeviceIdType.MESH)

    def gh_copy(d):
        return pltpu.make_async_remote_copy(
            src_ref=comp, dst_ref=ghr.at[me_s], send_sem=gh_send, recv_sem=gh_recv,
            device_id={"grp": me_g, "sub": sub_peer(d)}, device_id_type=pl.DeviceIdType.MESH)

    @pl.loop(1, n_grp)
    def _(d):
        slot_copy(d).start()

    @pl.loop(1, n_sub)
    def _(d):
        own_copy(d).start()

    def iota(shape, dim):
        return lax.broadcasted_iota(I32, shape, dim)

    named = jnp.where(gv_ref[...] < 128, 1.0, 0.0)
    named = jnp.broadcast_to(named, (8, n_grp * 10)).astype(BF)
    slots = (n_grp * 10, 128)
    first = jnp.where(iota(slots, 0) == 10 * iota(slots, 1), 1.0, 0.0).astype(BF)
    near = jnp.dot(named, first, preferred_element_type=F32)
    square = (128, 128)
    below = jnp.where(iota(square, 0) < iota(square, 1), 1.0, 0.0).astype(BF)
    rank = jnp.dot(near.astype(BF), below, preferred_element_type=F32)
    rank_out[...] = rank.astype(I32)
    value = ((rank + 1.0) * near).astype(BF)
    wide = (128, n_grp * 8)
    copies = jnp.where(iota(wide, 0) == (iota(wide, 1) >> 3), 1.0, 0.0).astype(BF)
    value = jnp.dot(value, copies, preferred_element_type=F32)[0:1]
    k = iota((1, n_grp * 8), 1) & 7
    place = jnp.where((k < 5) & (value > 0.5), (value - 1.0) * 5.0 + k.astype(F32), -1.0)
    rows = iota((GH_ROWS, n_grp * 8), 0).astype(F32)
    hot[...] = jnp.where(rows == place, 1.0, 0.0).astype(BF)

    def all_slots(ref):
        return ref.at[pl.ds(0, n_grp - 1)]

    every_slot = pltpu.make_async_remote_copy(
        src_ref=all_slots(send), dst_ref=all_slots(recv), send_sem=slot_send, recv_sem=slot_recv,
        device_id={"grp": grp_peer(1), "sub": me_s}, device_id_type=pl.DeviceIdType.MESH)
    every_slot.wait_recv()
    got = recv[...].astype(F32).reshape(n_grp * 8, 128).astype(BF)
    packed_ghosts = jnp.dot(hot[...], got, preferred_element_type=F32).astype(BF)
    comp[...] = packed_ghosts
    ghr[me_s] = packed_ghosts

    @pl.loop(1, n_sub)
    def _(d):
        gh_copy(d).start()

    def every(ref, src, s_sem, r_sem):
        part = ref.at[pl.ds(0, n_sub - 1)]
        return pltpu.make_async_remote_copy(
            src_ref=part, dst_ref=part, send_sem=s_sem, recv_sem=r_sem,
            device_id={"grp": me_g, "sub": sub_peer(1)}, device_id_type=pl.DeviceIdType.MESH)

    every_own = every(ownr, own, own_send, own_recv)
    every_own.wait_recv()
    own_out[...] = ownr[...]
    every_slot.wait_send()
    every_own.wait_send()
    every_gh = every(ghr, comp, gh_send, gh_recv)
    every_gh.wait_recv()
    gh_out[...] = ghr[...]
    every_gh.wait_send()


def exchange(ghost_map, x, u, p, n_grp, n_sub):
    ne = u.shape[0]
    dma = pltpu.SemaphoreType.DMA
    return pl.pallas_call(
        functools.partial(exchange_kernel, n_grp, n_sub),
        out_shape=(
            jax.ShapeDtypeStruct((n_sub, 64, 128), BF),
            jax.ShapeDtypeStruct((n_sub, GH_ROWS, 128), BF),
            jax.ShapeDtypeStruct((8, 128), I32),
        ),
        in_specs=[pl.BlockSpec(memory_space=pltpu.SMEM)] + [VM] * 4,
        out_specs=(VM, VM, VM),
        scratch_shapes=[
            pltpu.VMEM((pl.cdiv(ne, 128), ne * 8, 128), F32),
            pltpu.VMEM((136, 128), F32),
            pltpu.VMEM((n_grp, 8, 128), F32),
            pltpu.VMEM((n_grp, 8, 128), BF),
            pltpu.VMEM((n_grp, 8, 128), BF),
            pltpu.VMEM((64, 128), BF),
            pltpu.VMEM((n_sub, 64, 128), BF),
            pltpu.VMEM((GH_ROWS, 128), BF),
            pltpu.VMEM((n_sub, GH_ROWS, 128), BF),
            pltpu.VMEM((GH_ROWS, n_grp * 8), BF),
        ] + [dma] * 6,
        compiler_params=pltpu.CompilerParams(
            collective_id=0, has_side_effects=True, vmem_limit_bytes=24 * 2**20),
    )(ghost_map, ghost_map, x, u, p)

BUF = 3


def m2l_kernel(nbr_ref, rank_ref, own_ref, gh_ref, t_ref, e_ref, d_ref, out_ref,
               tab, idxv, sem, acc, dsc, *bufs):
    sms, sts = bufs[:BUF], bufs[BUF:]
    offs = nbr_ref.shape[0]
    full = offs // 8
    tail = offs - 8 * full
    zero_row = 1024 + 16 * GH_ROWS
    ranks = rank_ref[...]

    def place(v):
        rank = ranks[: v.shape[0]]
        w = jnp.maximum(v - 1024, 0)
        s = (w * 8739) >> 23
        u = w - s * 960
        g = (u * 6554) >> 16
        k = u - g * 10
        r = jnp.take_along_axis(rank, g, axis=1)
        half = jnp.where(k >= 5, 1, 0)
        row = 1024 + s * (2 * GH_ROWS) + half * GH_ROWS + r * 5 + (k - 5 * half)
        row = jnp.where(v < 1024, v, row)
        return jnp.where(v >= 8704, zero_row, row)

    idxv[pl.ds(0, 8), :] = jnp.concatenate(
        [place(nbr_ref[pl.ds(0, tail), :]), jnp.full((8 - tail, 128), zero_row, I32)], axis=0)
    for i in range(full):
        idxv[pl.ds(8 * i + 8, 8), :] = place(nbr_ref[pl.ds(tail + 8 * i, 8), :])

    def fetch(i, b):
        return pltpu.make_async_copy(idxv.at[pl.ds(pl.multiple_of(i * 8, 8), 8)], sms[b], sem.at[b])

    for b in range(BUF):
        fetch(b, b).start()
    lo64 = lax.broadcasted_iota(I32, (1, 128), 1) < 64

    def spread(src, base, rows):
        x = src.astype(F32)
        y = pltpu.roll(x, 64, 1)
        tab[pl.ds(pl.multiple_of(base, 8), rows), :] = jnp.where(lo64, x, y)
        tab[pl.ds(pl.multiple_of(base + rows, 8), rows), :] = jnp.where(lo64, y, x)

    for s in range(8):
        spread(own_ref[s], s * 128, 64)
        spread(gh_ref[s], 1024 + s * 2 * GH_ROWS, GH_ROWS)
    tab[pl.ds(zero_row, 8), :] = jnp.zeros((8, 128), F32)
    acc[...] = jnp.zeros_like(acc)

    def gather(sm, st, rows):
        for o in range(0, rows, 2):
            for t in range(128):
                st[o // 2, pl.ds(t, 1), :] = jnp.where(
                    lo64, tab[pl.ds(sm[o, t], 1), :], tab[pl.ds(sm[o + 1, t], 1), :])

    def product(first, st, rows):
        p = jnp.concatenate([st[j] for j in range(rows // 2)], axis=1).astype(BF)
        tt = t_ref[:, pl.ds(pl.multiple_of(first * 64, 256), rows * 64)]
        acc[...] += lax.dot_general(tt, p, NT, preferred_element_type=F32)

    fetch(0, 0).wait()
    gather(sms[0], sts[0], tail)
    product(0, sts[0], tail)
    fetch(BUF, 0).start()

    @pl.loop(0, full // BUF)
    def _(j):
        for c in range(BUF):
            b = (c + 1) % BUF
            i = BUF * j + c
            fetch(i + 1, b).wait()
            gather(sms[b], sts[b], 8)
            product(tail + 8 * i, sts[b], 8)

            @pl.when(i + 1 + BUF <= full)
            def _():
                fetch(i + 1 + BUF, b).start()

    lc = acc[...].astype(BF)
    lm = jnp.dot(e_ref[...], lc, preferred_element_type=F32).astype(BF)
    ne = d_ref.shape[0]
    dsc[...] = jnp.dot(d_ref[...].reshape(ne * 8, ne), lm, preferred_element_type=F32)
    for c in range(8):
        out_ref[:, c * 128 : (c + 1) * 128] = dsc[pl.ds(c, ne, stride=8), :].astype(BF)


def m2l(nbr, rank, own, gh, t, e, d):
    ne = d.shape[0]
    return pl.pallas_call(
        m2l_kernel,
        out_shape=jax.ShapeDtypeStruct((ne, 1024), BF),
        in_specs=[VM] * 7,
        out_specs=VM,
        scratch_shapes=[
            pltpu.VMEM((1024 + 16 * GH_ROWS + 8, 128), F32),
            pltpu.VMEM((320, 128), I32),
            pltpu.SemaphoreType.DMA((BUF,)),
            pltpu.VMEM((64, 128), F32),
            pltpu.VMEM((ne * 8, 128), F32),
            *[pltpu.SMEM((8, 128), I32)] * BUF,
            *[pltpu.VMEM((4, 128, 128), F32)] * BUF,
        ],
        compiler_params=pltpu.CompilerParams(vmem_limit_bytes=24 * 2**20),
    )(nbr, rank, own, gh, t, e, d)


def on_device(
    child_moments,
    upward_matrix,
    project_matrix,
    transfer_matrix,
    expand_matrix,
    downward_matrix,
    neighbour_list,
    ghost_map,
):
    own, ghosts, ranks = exchange(ghost_map, child_moments, upward_matrix, project_matrix,
                                  lax.axis_size("grp"), lax.axis_size("sub"))
    return m2l(neighbour_list, ranks, own, ghosts, transfer_matrix, expand_matrix, downward_matrix)


def solution(mesh):
    return jax.shard_map(
        on_device,
        mesh=mesh,
        in_specs=(
            P(None, ("grp", "sub")),
            P(),
            P(),
            P(),
            P(),
            P(),
            P(None, ("grp", "sub")),
            P(("grp", "sub"), None),
        ),
        out_specs=P(None, ("grp", "sub")),
        check_vma=False,
    )
```

```python
import functools
import jax
import jax.numpy as jnp
from jax import lax
from jax.experimental import pallas as pl
from jax.experimental.pallas import tpu as pltpu

from jax.sharding import PartitionSpec as P

F32, BF, I32 = jnp.float32, jnp.bfloat16, jnp.int32
NT = (((1,), (1,)), ((), ()))
VM = pl.BlockSpec(memory_space=pltpu.VMEM)
HB = pl.BlockSpec(memory_space=pltpu.HBM)
GH_ROWS = 136
ZERO_ROW = 1024 + 16 * GH_ROWS


def place(v, rank):
    rank = rank[: v.shape[0]]
    w = jnp.maximum(v - 1024, 0)
    s = (w * 8739) >> 23
    u = w - s * 960
    g = (u * 6554) >> 16
    k = u - g * 10
    r = jnp.take_along_axis(rank, g, axis=1)
    half = jnp.where(k >= 5, 1, 0)
    row = 1024 + s * (2 * GH_ROWS) + half * GH_ROWS + r * 5 + (k - 5 * half)
    row = jnp.where(v < 1024, v, row)
    return jnp.where(v >= 8704, ZERO_ROW, row)


def exchange_kernel(n_grp, n_sub, g_hbm, x_hbm, u_hbm, p_hbm, n_hbm, own_out, gh_out, idx_out,
                    gs_ref, gv_ref, x_ref, u_ref, p_ref, nbr_ref, in_sem, uf, tab, sf, send, recv, own, ownr, comp, ghr, hot,
                    own_send, own_recv, slot_send, slot_recv, gh_send, gh_recv):
    me_g, me_s = lax.axis_index("grp"), lax.axis_index("sub")
    ne = u_ref.shape[0]
    barrier = pltpu.get_barrier_semaphore()

    def grp_peer(d):
        return lax.rem(me_g + d, n_grp)

    def sub_peer(d):
        return lax.rem(me_s + d, n_sub)

    @pl.loop(1, n_grp)
    def _(d):
        pl.semaphore_signal(barrier, inc=1, device_id={"grp": grp_peer(d), "sub": me_s},
                            device_id_type=pl.DeviceIdType.MESH)

    @pl.loop(1, n_sub)
    def _(d):
        pl.semaphore_signal(barrier, inc=1, device_id={"grp": me_g, "sub": sub_peer(d)},
                            device_id_type=pl.DeviceIdType.MESH)

    loads = [
        pltpu.make_async_copy(src, dst, in_sem.at[n])
        for n, (src, dst) in enumerate([(u_hbm, u_ref), (x_hbm, x_ref), (g_hbm, gs_ref),
                                        (p_hbm, p_ref), (g_hbm, gv_ref), (n_hbm, nbr_ref)])
    ]
    for load in loads:
        load.start()
    loads[0].wait()
    flat = u_ref[...].reshape(ne * 8, ne).astype(F32)
    starts = range(0, ne, 128)
    for n, at in enumerate(starts):
        width = min(128, ne - at)
        uf[n, :, pl.ds(0, width)] = flat[:, at : at + width]
    loads[1].wait()
    loads[3].wait()
    total = jnp.zeros((ne, 128), F32)
    for c in range(8):
        tiles = [uf[n, pl.ds(c, ne, stride=8), :].astype(BF) for n in range(len(starts))]
        tiles[-1] = tiles[-1][:, : ne - starts[-1]]
        total += jnp.dot(jnp.concatenate(tiles, axis=1), x_ref[:, c * 128 : (c + 1) * 128],
                         preferred_element_type=F32)
    parent = total.astype(BF)
    twice = jnp.concatenate([p_ref[...], p_ref[...]], axis=0)
    packed = jnp.dot(twice, parent, preferred_element_type=F32).T.astype(BF).astype(F32)
    lo64 = lax.broadcasted_iota(I32, (1, 128), 1) < 64
    tab[pl.ds(0, 128), :] = packed
    tab[pl.ds(128, 8), :] = jnp.zeros((8, 128), F32)
    mine = jnp.where(lo64, packed[0:64], packed[64:128]).astype(BF)
    own[...] = mine
    ownr[me_s] = mine
    sf[...] = jnp.zeros_like(sf)
    loads[2].wait()

    @pl.loop(0, n_grp)
    def _(g):
        for k in range(5):
            sf[g, pl.ds(k, 1), :] = jnp.where(lo64, tab[pl.ds(gs_ref[0, g * 10 + k], 1), :],
                                              tab[pl.ds(gs_ref[0, g * 10 + 5 + k], 1), :])

    send[...] = sf[...].astype(BF)
    recv[me_g] = send[me_g]
    pl.semaphore_wait(barrier, n_grp + n_sub - 2)

    def own_copy(d):
        return pltpu.make_async_remote_copy(
            src_ref=own, dst_ref=ownr.at[me_s], send_sem=own_send, recv_sem=own_recv,
            device_id={"grp": me_g, "sub": sub_peer(d)}, device_id_type=pl.DeviceIdType.MESH)

    def slot_copy(d):
        g = grp_peer(d)
        return pltpu.make_async_remote_copy(
            src_ref=send.at[g], dst_ref=recv.at[me_g], send_sem=slot_send, recv_sem=slot_recv,
            device_id={"grp": g, "sub": me_s}, device_id_type=pl.DeviceIdType.MESH)

    def gh_copy(d):
        return pltpu.make_async_remote_copy(
            src_ref=comp, dst_ref=ghr.at[me_s], send_sem=gh_send, recv_sem=gh_recv,
            device_id={"grp": me_g, "sub": sub_peer(d)}, device_id_type=pl.DeviceIdType.MESH)

    @pl.loop(1, n_grp)
    def _(d):
        slot_copy(d).start()

    @pl.loop(1, n_sub)
    def _(d):
        own_copy(d).start()

    def iota(shape, dim):
        return lax.broadcasted_iota(I32, shape, dim)

    loads[4].wait()
    named = jnp.where(gv_ref[...] < 128, 1.0, 0.0)
    named = jnp.broadcast_to(named, (8, n_grp * 10)).astype(BF)
    slots = (n_grp * 10, 128)
    first = jnp.where(iota(slots, 0) == 10 * iota(slots, 1), 1.0, 0.0).astype(BF)
    near = jnp.dot(named, first, preferred_element_type=F32)
    square = (128, 128)
    below = jnp.where(iota(square, 0) < iota(square, 1), 1.0, 0.0).astype(BF)
    rank = jnp.dot(near.astype(BF), below, preferred_element_type=F32)
    ranks = rank.astype(I32)
    value = ((rank + 1.0) * near).astype(BF)
    wide = (128, n_grp * 8)
    copies = jnp.where(iota(wide, 0) == (iota(wide, 1) >> 3), 1.0, 0.0).astype(BF)
    value = jnp.dot(value, copies, preferred_element_type=F32)[0:1]
    k = iota((1, n_grp * 8), 1) & 7
    target = jnp.where((k < 5) & (value > 0.5), (value - 1.0) * 5.0 + k.astype(F32), -1.0)
    rows = iota((GH_ROWS, n_grp * 8), 0).astype(F32)
    hot[...] = jnp.where(rows == target, 1.0, 0.0).astype(BF)

    loads[5].wait()
    offs = nbr_ref.shape[0]
    tail = offs % 8
    idx_out[pl.ds(0, 8), :] = jnp.concatenate(
        [place(nbr_ref[pl.ds(0, tail), :], ranks), jnp.full((8 - tail, 128), ZERO_ROW, I32)], axis=0)
    for i in range(offs // 8):
        idx_out[pl.ds(8 * i + 8, 8), :] = place(nbr_ref[pl.ds(tail + 8 * i, 8), :], ranks)

    def all_slots(ref):
        return ref.at[pl.ds(0, n_grp - 1)]

    every_slot = pltpu.make_async_remote_copy(
        src_ref=all_slots(send), dst_ref=all_slots(recv), send_sem=slot_send, recv_sem=slot_recv,
        device_id={"grp": grp_peer(1), "sub": me_s}, device_id_type=pl.DeviceIdType.MESH)
    every_slot.wait_recv()
    got = recv[...].astype(F32).reshape(n_grp * 8, 128).astype(BF)
    packed_ghosts = jnp.dot(hot[...], got, preferred_element_type=F32).astype(BF)
    comp[...] = packed_ghosts
    ghr[me_s] = packed_ghosts

    @pl.loop(1, n_sub)
    def _(d):
        gh_copy(d).start()

    def every(ref, src, s_sem, r_sem):
        part = ref.at[pl.ds(0, n_sub - 1)]
        return pltpu.make_async_remote_copy(
            src_ref=part, dst_ref=part, send_sem=s_sem, recv_sem=r_sem,
            device_id={"grp": me_g, "sub": sub_peer(1)}, device_id_type=pl.DeviceIdType.MESH)

    every_own = every(ownr, own, own_send, own_recv)
    every_own.wait_recv()
    own_out[...] = ownr[...]
    every_slot.wait_send()
    every_own.wait_send()
    every_gh = every(ghr, comp, gh_send, gh_recv)
    every_gh.wait_recv()
    gh_out[...] = ghr[...]
    every_gh.wait_send()


def exchange(ghost_map, x, u, p, nbr, n_grp, n_sub):
    ne = u.shape[0]
    dma = pltpu.SemaphoreType.DMA
    return pl.pallas_call(
        functools.partial(exchange_kernel, n_grp, n_sub),
        out_shape=(
            jax.ShapeDtypeStruct((n_sub, 64, 128), BF),
            jax.ShapeDtypeStruct((n_sub, GH_ROWS, 128), BF),
            jax.ShapeDtypeStruct((320, 128), I32),
        ),
        in_specs=[HB] * 5,
        out_specs=(VM, VM, VM),
        scratch_shapes=[
            pltpu.SMEM(ghost_map.shape, I32),
            pltpu.VMEM(ghost_map.shape, I32),
            pltpu.VMEM(x.shape, BF),
            pltpu.VMEM(u.shape, BF),
            pltpu.VMEM(p.shape, BF),
            pltpu.VMEM(nbr.shape, I32),
            dma((6,)),
            pltpu.VMEM((pl.cdiv(ne, 128), ne * 8, 128), F32),
            pltpu.VMEM((136, 128), F32),
            pltpu.VMEM((n_grp, 8, 128), F32),
            pltpu.VMEM((n_grp, 8, 128), BF),
            pltpu.VMEM((n_grp, 8, 128), BF),
            pltpu.VMEM((64, 128), BF),
            pltpu.VMEM((n_sub, 64, 128), BF),
            pltpu.VMEM((GH_ROWS, 128), BF),
            pltpu.VMEM((n_sub, GH_ROWS, 128), BF),
            pltpu.VMEM((GH_ROWS, n_grp * 8), BF),
        ] + [dma] * 6,
        compiler_params=pltpu.CompilerParams(
            collective_id=0, has_side_effects=True, vmem_limit_bytes=24 * 2**20),
    )(*[pltpu.with_memory_space_constraint(a, pltpu.HBM) for a in (ghost_map, x, u, p, nbr)])

BUF = 3


def m2l_kernel(idx_ref, own_ref, gh_ref, t_ref, e_hbm, d_hbm, out_ref,
               tab, e_ref, d_ref, late_sem, sem, acc, dsc, *bufs):
    sms, sts = bufs[:BUF], bufs[BUF:]
    full = idx_ref.shape[0] // 8 - 1
    tail = t_ref.shape[1] // 64 - 8 * full
    e_load = pltpu.make_async_copy(e_hbm, e_ref, late_sem.at[0])
    d_load = pltpu.make_async_copy(d_hbm, d_ref, late_sem.at[1])
    e_load.start()
    d_load.start()

    def fetch(i, b):
        return pltpu.make_async_copy(idx_ref.at[pl.ds(pl.multiple_of(i * 8, 8), 8)], sms[b], sem.at[b])

    for b in range(BUF):
        fetch(b, b).start()
    lo64 = lax.broadcasted_iota(I32, (1, 128), 1) < 64

    def spread(src, base, rows):
        x = src.astype(F32)
        y = pltpu.roll(x, 64, 1)
        tab[pl.ds(pl.multiple_of(base, 8), rows), :] = jnp.where(lo64, x, y)
        tab[pl.ds(pl.multiple_of(base + rows, 8), rows), :] = jnp.where(lo64, y, x)

    for s in range(8):
        spread(own_ref[s], s * 128, 64)
        spread(gh_ref[s], 1024 + s * 2 * GH_ROWS, GH_ROWS)
    tab[pl.ds(ZERO_ROW, 8), :] = jnp.zeros((8, 128), F32)
    acc[...] = jnp.zeros_like(acc)

    def gather(sm, st, rows):
        for o in range(0, rows, 2):
            for t in range(128):
                st[o // 2, pl.ds(t, 1), :] = jnp.where(
                    lo64, tab[pl.ds(sm[o, t], 1), :], tab[pl.ds(sm[o + 1, t], 1), :])

    def product(first, st, rows):
        p = jnp.concatenate([st[j] for j in range(rows // 2)], axis=1).astype(BF)
        tt = t_ref[:, pl.ds(pl.multiple_of(first * 64, 256), rows * 64)]
        acc[...] += lax.dot_general(tt, p, NT, preferred_element_type=F32)

    fetch(0, 0).wait()
    gather(sms[0], sts[0], tail)
    product(0, sts[0], tail)
    fetch(BUF, 0).start()

    @pl.loop(0, full // BUF)
    def _(j):
        for c in range(BUF):
            b = (c + 1) % BUF
            i = BUF * j + c
            fetch(i + 1, b).wait()
            gather(sms[b], sts[b], 8)
            product(tail + 8 * i, sts[b], 8)

            @pl.when(i + 1 + BUF <= full)
            def _():
                fetch(i + 1 + BUF, b).start()

    lc = acc[...].astype(BF)
    e_load.wait()
    lm = lax.dot_general(e_ref[...], lc, (((0,), (0,)), ((), ())), preferred_element_type=F32).astype(BF)
    d_load.wait()
    ne = d_ref.shape[0]
    dsc[...] = jnp.dot(d_ref[...].reshape(ne * 8, ne), lm, preferred_element_type=F32)
    for c in range(8):
        out_ref[:, c * 128 : (c + 1) * 128] = dsc[pl.ds(c, ne, stride=8), :].astype(BF)


def m2l(idx, own, gh, t, e, d):
    ne = d.shape[0]
    return pl.pallas_call(
        m2l_kernel,
        out_shape=jax.ShapeDtypeStruct((ne, 1024), BF),
        in_specs=[pl.BlockSpec(memory_space=pl.ANY)] + [VM] * 3 + [HB] * 2,
        out_specs=VM,
        scratch_shapes=[
            pltpu.VMEM((1024 + 16 * GH_ROWS + 8, 128), F32),
            pltpu.VMEM(e.shape[::-1], BF),
            pltpu.VMEM(d.shape, BF),
            pltpu.SemaphoreType.DMA((2,)),
            pltpu.SemaphoreType.DMA((BUF,)),
            pltpu.VMEM((64, 128), F32),
            pltpu.VMEM((ne * 8, 128), F32),
            *[pltpu.SMEM((8, 128), I32)] * BUF,
            *[pltpu.VMEM((4, 128, 128), F32)] * BUF,
        ],
        compiler_params=pltpu.CompilerParams(vmem_limit_bytes=24 * 2**20),
    )(idx, own, gh, t, *[pltpu.with_memory_space_constraint(a, pltpu.HBM) for a in (e.T, d)])


def on_device(
    child_moments,
    upward_matrix,
    project_matrix,
    transfer_matrix,
    expand_matrix,
    downward_matrix,
    neighbour_list,
    ghost_map,
):
    own, ghosts, index = exchange(ghost_map, child_moments, upward_matrix, project_matrix,
                                  neighbour_list, lax.axis_size("grp"), lax.axis_size("sub"))
    return m2l(index, own, ghosts, transfer_matrix, expand_matrix, downward_matrix)


def solution(mesh):
    return jax.shard_map(
        on_device,
        mesh=mesh,
        in_specs=(
            P(None, ("grp", "sub")),
            P(),
            P(),
            P(),
            P(),
            P(),
            P(None, ("grp", "sub")),
            P(("grp", "sub"), None),
        ),
        out_specs=P(None, ("grp", "sub")),
        check_vma=False,
    )
```

```python
import functools
import jax
import jax.numpy as jnp
from jax import lax
from jax.experimental import pallas as pl
from jax.experimental.pallas import tpu as pltpu

from jax.sharding import PartitionSpec as P

F32, BF, I32 = jnp.float32, jnp.bfloat16, jnp.int32
NT = (((1,), (1,)), ((), ()))
VM = pl.BlockSpec(memory_space=pltpu.VMEM)
HB = pl.BlockSpec(memory_space=pltpu.HBM)
GH_ROWS = 136
ZERO_ROW = 1024 + 16 * GH_ROWS


def place(v, rank):
    rank = rank[: v.shape[0]]
    w = jnp.maximum(v - 1024, 0)
    s = (w * 8739) >> 23
    u = w - s * 960
    g = (u * 6554) >> 16
    k = u - g * 10
    r = jnp.take_along_axis(rank, g, axis=1)
    half = jnp.where(k >= 5, 1, 0)
    row = 1024 + s * (2 * GH_ROWS) + half * GH_ROWS + r * 5 + (k - 5 * half)
    row = jnp.where(v < 1024, v, row)
    return jnp.where(v >= 8704, ZERO_ROW, row)


def exchange_kernel(n_grp, n_sub, g_hbm, x_hbm, u_hbm, p_hbm, n_hbm, own_out, gh_out, idx_out,
                    gs_ref, gv_ref, x_ref, u_ref, p_ref, nbr_ref, in_sem, uf, tab, sf, send, recv, own, ownr, comp, ghr, hot,
                    own_send, own_recv, slot_send, slot_recv, gh_send, gh_recv):
    me_g, me_s = lax.axis_index("grp"), lax.axis_index("sub")
    ne = u_ref.shape[0]
    barrier = pltpu.get_barrier_semaphore()

    loads = [
        pltpu.make_async_copy(src, dst, in_sem.at[n])
        for n, (src, dst) in enumerate([(u_hbm, u_ref), (x_hbm, x_ref), (g_hbm, gs_ref),
                                        (p_hbm, p_ref), (g_hbm, gv_ref), (n_hbm, nbr_ref)])
    ]
    for load in loads:
        load.start()
    n_z = 12
    me_x, me_z, me_c = me_g // (2 * n_z), lax.rem(me_g // 2, n_z), lax.rem(me_g, 2)

    def for_grp_peers(act):
        n_x = n_grp // (2 * n_z)

        def row(step, last):
            half = (step + 1) // 2
            z = lax.rem(me_z + n_z // 2 + half * (1 - 2 * lax.rem(step, 2)) + n_z, n_z)
            for dx in sorted(range(n_x), key=lambda v: -min(v, n_x - v)):
                for dc in (1, 0):
                    if last and dx == 0 and dc == 0:
                        continue
                    x, c = lax.rem(me_x + dx, n_x), lax.rem(me_c + dc, 2)
                    act((x * n_z + z) * 2 + c)

        @pl.loop(0, n_z - 1)
        def _(step):
            row(step, False)

        row(jnp.int32(n_z - 1), True)

    def for_sub_peers(act):
        for d in sorted(range(1, n_sub), key=lambda v: -min(v, n_sub - v)):
            act(lax.rem(me_s + d, n_sub))

    def greet(g, s):
        pl.semaphore_signal(barrier, inc=1, device_id={"grp": g, "sub": s},
                            device_id_type=pl.DeviceIdType.MESH)

    for_grp_peers(lambda g: greet(g, me_s))
    for_sub_peers(lambda s: greet(me_g, s))
    loads[0].wait()
    flat = u_ref[...].reshape(ne * 8, ne).astype(F32)
    starts = range(0, ne, 128)
    for n, at in enumerate(starts):
        width = min(128, ne - at)
        uf[n, :, pl.ds(0, width)] = flat[:, at : at + width]
    loads[1].wait()
    loads[3].wait()
    total = jnp.zeros((ne, 128), F32)
    for c in range(8):
        tiles = [uf[n, pl.ds(c, ne, stride=8), :].astype(BF) for n in range(len(starts))]
        tiles[-1] = tiles[-1][:, : ne - starts[-1]]
        total += jnp.dot(jnp.concatenate(tiles, axis=1), x_ref[:, c * 128 : (c + 1) * 128],
                         preferred_element_type=F32)
    parent = total.astype(BF)
    twice = jnp.concatenate([p_ref[...], p_ref[...]], axis=0)
    packed = jnp.dot(twice, parent, preferred_element_type=F32).T.astype(BF).astype(F32)
    lo64 = lax.broadcasted_iota(I32, (1, 128), 1) < 64
    tab[pl.ds(0, 128), :] = packed
    tab[pl.ds(128, 8), :] = jnp.zeros((8, 128), F32)
    mine = jnp.where(lo64, packed[0:64], packed[64:128]).astype(BF)
    own[...] = mine
    ownr[me_s] = mine
    sf[...] = jnp.zeros_like(sf)
    loads[2].wait()

    @pl.loop(0, n_grp // 8)
    def _(step):
        for n in range(8):
            g = step * 8 + n
            for k in range(5):
                sf[g, pl.ds(k, 1), :] = jnp.where(lo64, tab[pl.ds(gs_ref[0, g * 10 + k], 1), :],
                                                  tab[pl.ds(gs_ref[0, g * 10 + 5 + k], 1), :])

    for j in range(3):
        send[:, j] = sf[:, 2 * j : 2 * j + 2, :].astype(BF)
    recv[me_g] = send[me_g]
    pl.semaphore_wait(barrier, n_grp + n_sub - 2)

    def own_copy(s):
        return pltpu.make_async_remote_copy(
            src_ref=own, dst_ref=ownr.at[me_s], send_sem=own_send, recv_sem=own_recv,
            device_id={"grp": me_g, "sub": s}, device_id_type=pl.DeviceIdType.MESH)

    def slot_copy(g):
        return pltpu.make_async_remote_copy(
            src_ref=send.at[g], dst_ref=recv.at[me_g], send_sem=slot_send, recv_sem=slot_recv,
            device_id={"grp": g, "sub": me_s}, device_id_type=pl.DeviceIdType.MESH)

    def gh_copy(s):
        return pltpu.make_async_remote_copy(
            src_ref=comp, dst_ref=ghr.at[me_s], send_sem=gh_send, recv_sem=gh_recv,
            device_id={"grp": me_g, "sub": s}, device_id_type=pl.DeviceIdType.MESH)

    for_grp_peers(lambda g: slot_copy(g).start())
    for_sub_peers(lambda s: own_copy(s).start())

    def iota(shape, dim):
        return lax.broadcasted_iota(I32, shape, dim)

    loads[4].wait()
    named = jnp.where(gv_ref[...] < 128, 1.0, 0.0)
    named = jnp.broadcast_to(named, (8, n_grp * 10)).astype(BF)
    slots = (n_grp * 10, 128)
    first = jnp.where(iota(slots, 0) == 10 * iota(slots, 1), 1.0, 0.0).astype(BF)
    near = jnp.dot(named, first, preferred_element_type=F32)
    square = (128, 128)
    below = jnp.where(iota(square, 0) < iota(square, 1), 1.0, 0.0).astype(BF)
    rank = jnp.dot(near.astype(BF), below, preferred_element_type=F32)
    ranks = rank.astype(I32)
    value = ((rank + 1.0) * near).astype(BF)
    wide = (128, n_grp * 8)
    copies = jnp.where(iota(wide, 0) == (iota(wide, 1) >> 3), 1.0, 0.0).astype(BF)
    value = jnp.dot(value, copies, preferred_element_type=F32)[0:1]
    k = iota((1, n_grp * 8), 1) & 7
    target = jnp.where((k < 5) & (value > 0.5), (value - 1.0) * 5.0 + k.astype(F32), -1.0)
    rows = iota((GH_ROWS, n_grp * 8), 0).astype(F32)
    hot[...] = jnp.where(rows == target, 1.0, 0.0).astype(BF)

    loads[5].wait()
    offs = nbr_ref.shape[0]
    tail = offs % 16
    idx_out[pl.ds(0, 8), :] = place(nbr_ref[pl.ds(0, 8), :], ranks)
    idx_out[pl.ds(8, 8), :] = jnp.concatenate(
        [place(nbr_ref[pl.ds(8, tail - 8), :], ranks), jnp.full((16 - tail, 128), ZERO_ROW, I32)], axis=0)
    for i in range((offs - tail) // 8):
        idx_out[pl.ds(8 * i + 16, 8), :] = place(nbr_ref[pl.ds(tail + 8 * i, 8), :], ranks)

    def all_slots(ref):
        return ref.at[pl.ds(0, n_grp - 1)]

    every_slot = pltpu.make_async_remote_copy(
        src_ref=all_slots(send), dst_ref=all_slots(recv), send_sem=slot_send, recv_sem=slot_recv,
        device_id={"grp": lax.rem(me_g + 1, n_grp), "sub": me_s}, device_id_type=pl.DeviceIdType.MESH)
    every_slot.wait_recv()
    for j in range(3):
        sf[:, 2 * j : 2 * j + 2, :] = recv[:, j].astype(F32)
    got = sf[...].reshape(n_grp * 8, 128).astype(BF)
    packed_ghosts = jnp.dot(hot[...], got, preferred_element_type=F32).astype(BF)
    comp[...] = packed_ghosts
    ghr[me_s] = packed_ghosts

    for_sub_peers(lambda s: gh_copy(s).start())

    def every(ref, src, s_sem, r_sem):
        part = ref.at[pl.ds(0, n_sub - 1)]
        return pltpu.make_async_remote_copy(
            src_ref=part, dst_ref=part, send_sem=s_sem, recv_sem=r_sem,
            device_id={"grp": me_g, "sub": lax.rem(me_s + 1, n_sub)}, device_id_type=pl.DeviceIdType.MESH)

    every_own = every(ownr, own, own_send, own_recv)
    every_own.wait_recv()
    own_out[...] = ownr[...]
    every_slot.wait_send()
    every_own.wait_send()
    every_gh = every(ghr, comp, gh_send, gh_recv)
    every_gh.wait_recv()
    gh_out[...] = ghr[...]
    every_gh.wait_send()


def exchange(ghost_map, x, u, p, nbr, n_grp, n_sub):
    ne = u.shape[0]
    dma = pltpu.SemaphoreType.DMA
    return pl.pallas_call(
        functools.partial(exchange_kernel, n_grp, n_sub),
        out_shape=(
            jax.ShapeDtypeStruct((n_sub, 64, 128), BF),
            jax.ShapeDtypeStruct((n_sub, GH_ROWS, 128), BF),
            jax.ShapeDtypeStruct((320, 128), I32),
        ),
        in_specs=[HB] * 5,
        out_specs=(VM, VM, VM),
        scratch_shapes=[
            pltpu.SMEM(ghost_map.shape, I32),
            pltpu.VMEM(ghost_map.shape, I32),
            pltpu.VMEM(x.shape, BF),
            pltpu.VMEM(u.shape, BF),
            pltpu.VMEM(p.shape, BF),
            pltpu.VMEM(nbr.shape, I32),
            dma((6,)),
            pltpu.VMEM((pl.cdiv(ne, 128), ne * 8, 128), F32),
            pltpu.VMEM((136, 128), F32),
            pltpu.VMEM((n_grp, 8, 128), F32),
            pltpu.VMEM((n_grp, 3, 2, 128), BF),
            pltpu.VMEM((n_grp, 3, 2, 128), BF),
            pltpu.VMEM((64, 128), BF),
            pltpu.VMEM((n_sub, 64, 128), BF),
            pltpu.VMEM((GH_ROWS, 128), BF),
            pltpu.VMEM((n_sub, GH_ROWS, 128), BF),
            pltpu.VMEM((GH_ROWS, n_grp * 8), BF),
        ] + [dma] * 6,
        compiler_params=pltpu.CompilerParams(
            collective_id=0, has_side_effects=True, vmem_limit_bytes=24 * 2**20),
    )(*[pltpu.with_memory_space_constraint(a, pltpu.HBM) for a in (ghost_map, x, u, p, nbr)])

BUF = 3


def m2l_kernel(idx_ref, own_ref, gh_ref, t_ref, e_hbm, d_hbm, out_ref,
               tab, flat, e_ref, d_ref, late_sem, sem, acc, dsc, *bufs):
    sms, sts = bufs[:BUF], bufs[BUF:]
    chunks = idx_ref.shape[0] // 16
    tiles = tab.shape[0] // 256
    e_load = pltpu.make_async_copy(e_hbm, e_ref, late_sem.at[0])
    d_load = pltpu.make_async_copy(d_hbm, d_ref, late_sem.at[1])
    e_load.start()
    d_load.start()

    def fetch(i, b):
        return pltpu.make_async_copy(idx_ref.at[pl.ds(pl.multiple_of(i * 16, 16), 8)], sms[b], sem.at[b])

    for b in range(BUF):
        fetch(b, b).start()
    lo64 = lax.broadcasted_iota(I32, (1, 128), 1) < 64

    def spread(src, base, rows):
        x = src.astype(F32)
        y = pltpu.roll(x, 64, 1)
        tab[pl.ds(base, rows), :] = jnp.where(lo64, x, y)
        tab[pl.ds(base + rows, rows), :] = jnp.where(lo64, y, x)

    for s in range(8):
        spread(own_ref[s], s * 128, 64)
        spread(gh_ref[s], 1024 + s * 2 * GH_ROWS, GH_ROWS)
    rest = tab.shape[0] - ZERO_ROW
    tab[pl.ds(ZERO_ROW, rest), :] = jnp.zeros((rest, 128), F32)
    for h in range(tiles):
        flat[pl.ds(h * 64, 64), :] = tab[pl.ds(h * 256, 256), :].T[:64].astype(BF)
    acc[...] = jnp.zeros_like(acc)

    def by_rows(sm, st, first):
        for o in range(0, 8, 2):
            for t in range(128):
                st[o // 2, pl.ds(t, 1), :] = jnp.where(
                    lo64, tab[pl.ds(sm[o, t], 1), :], tab[pl.ds(sm[o + 1, t], 1), :])
        p = jnp.concatenate([st[j] for j in range(4)], axis=1).astype(BF)
        return lax.dot_general(t_ref[:, pl.ds(pl.multiple_of(first * 64, 256), 512)], p, NT,
                               preferred_element_type=F32)

    def by_select(row, first, count):
        block = idx_ref[pl.ds(pl.multiple_of(row, 8), 8), :]
        deep = lax.broadcasted_iota(I32, (256, 256), 0)
        parts = []
        for o in range(0, count, 2):
            v = jnp.concatenate([block[o : o + 1], block[o + 1 : o + 2]], axis=1)
            low, high = v & 255, v >> 8
            hot = jnp.where(deep == low, 1.0, 0.0).astype(BF)
            every = jnp.dot(flat[...], hot, preferred_element_type=F32)
            got = jnp.where(high == 0, every[0:64], 0.0)
            for h in range(1, tiles):
                got = jnp.where(high == h, every[h * 64 : h * 64 + 64], got)
            got = got.astype(BF)
            parts += [got[:, :128], got[:, 128:]]
        return jnp.dot(t_ref[:, pl.ds(pl.multiple_of(first * 64, 256), count * 64)],
                       jnp.concatenate(parts, axis=0), preferred_element_type=F32)

    def chunk(i, b, first, count=8):
        fetch(i, b).wait()
        acc[...] += by_rows(sms[b], sts[b], first) + by_select(16 * i + 8, first + 8, count)

    tail = t_ref.shape[1] // 64 - 16 * (chunks - 1)
    chunk(0, 0, 0, tail - 8)
    fetch(BUF, 0).start()
    chunk(1, 1, tail)
    fetch(BUF + 1, 1).start()

    @pl.loop(0, (chunks - 2) // BUF)
    def _(j):
        for c in range(BUF):
            b = (c + 2) % BUF
            i = BUF * j + c + 2
            chunk(i, b, tail + 16 * (i - 1))

            @pl.when(i + BUF < chunks)
            def _():
                fetch(i + BUF, b).start()

    lc = acc[...].astype(BF)
    e_load.wait()
    lm = lax.dot_general(e_ref[...], lc, (((0,), (0,)), ((), ())), preferred_element_type=F32).astype(BF)
    d_load.wait()
    ne = d_ref.shape[0]
    dsc[...] = jnp.dot(d_ref[...].reshape(ne * 8, ne), lm, preferred_element_type=F32)
    for c in range(8):
        out_ref[:, c * 128 : (c + 1) * 128] = dsc[pl.ds(c, ne, stride=8), :].astype(BF)


def m2l(idx, own, gh, t, e, d):
    ne = d.shape[0]
    table = pl.cdiv(ZERO_ROW + 1, 256) * 256
    return pl.pallas_call(
        m2l_kernel,
        out_shape=jax.ShapeDtypeStruct((ne, 1024), BF),
        in_specs=[VM] * 4 + [HB] * 2,
        out_specs=VM,
        scratch_shapes=[
            pltpu.VMEM((table, 128), F32),
            pltpu.VMEM((table // 4, 256), BF),
            pltpu.VMEM(e.shape[::-1], BF),
            pltpu.VMEM(d.shape, BF),
            pltpu.SemaphoreType.DMA((2,)),
            pltpu.SemaphoreType.DMA((BUF,)),
            pltpu.VMEM((64, 128), F32),
            pltpu.VMEM((ne * 8, 128), F32),
            *[pltpu.SMEM((8, 128), I32)] * BUF,
            *[pltpu.VMEM((4, 128, 128), F32)] * BUF,
        ],
        compiler_params=pltpu.CompilerParams(vmem_limit_bytes=24 * 2**20),
    )(idx, own, gh, t, *[pltpu.with_memory_space_constraint(a, pltpu.HBM) for a in (e.T, d)])


def on_device(
    child_moments,
    upward_matrix,
    project_matrix,
    transfer_matrix,
    expand_matrix,
    downward_matrix,
    neighbour_list,
    ghost_map,
):
    own, ghosts, index = exchange(ghost_map, child_moments, upward_matrix, project_matrix,
                                  neighbour_list, lax.axis_size("grp"), lax.axis_size("sub"))
    return m2l(index, own, ghosts, transfer_matrix, expand_matrix, downward_matrix)


def solution(mesh):
    return jax.shard_map(
        on_device,
        mesh=mesh,
        in_specs=(
            P(None, ("grp", "sub")),
            P(),
            P(),
            P(),
            P(),
            P(),
            P(None, ("grp", "sub")),
            P(("grp", "sub"), None),
        ),
        out_specs=P(None, ("grp", "sub")),
        check_vma=False,
    )
```

```python
import functools
import jax
import jax.numpy as jnp
from jax import lax
from jax.experimental import pallas as pl
from jax.experimental.pallas import tpu as pltpu

from jax.sharding import PartitionSpec as P

F32, BF, I32 = jnp.float32, jnp.bfloat16, jnp.int32
NT = (((1,), (1,)), ((), ()))
VM = pl.BlockSpec(memory_space=pltpu.VMEM)
HB = pl.BlockSpec(memory_space=pltpu.HBM)
GH_ROWS = 136
ZERO_ROW = 1024 + 16 * GH_ROWS


def place(v, rank):
    rank = rank[: v.shape[0]]
    w = jnp.maximum(v - 1024, 0)
    s = (w * 8739) >> 23
    u = w - s * 960
    g = (u * 6554) >> 16
    k = u - g * 10
    r = jnp.take_along_axis(rank, g, axis=1)
    half = jnp.where(k >= 5, 1, 0)
    row = 1024 + s * (2 * GH_ROWS) + half * GH_ROWS + r * 5 + (k - 5 * half)
    row = jnp.where(v < 1024, v, row)
    return jnp.where(v >= 8704, ZERO_ROW, row)


def exchange_kernel(n_grp, n_sub, g_hbm, x_hbm, u_hbm, p_hbm, n_hbm, own_out, gh_out, idx_out, part_out,
                    gs_ref, gv_ref, x_ref, u_ref, p_ref, nbr_ref, in_sem, uf, tab, sf, send, recv, own, ownr, comp, ghr, hot, own_flat,
                    own_send, own_recv, slot_send, slot_recv, gh_send, gh_recv):
    me_g, me_s = lax.axis_index("grp"), lax.axis_index("sub")
    ne = u_ref.shape[0]
    barrier = pltpu.get_barrier_semaphore()

    loads = [
        pltpu.make_async_copy(src, dst, in_sem.at[n])
        for n, (src, dst) in enumerate([(u_hbm, u_ref), (x_hbm, x_ref), (g_hbm, gs_ref),
                                        (p_hbm, p_ref), (g_hbm, gv_ref), (n_hbm, nbr_ref)])
    ]
    for load in loads:
        load.start()
    n_z = 12
    me_x, me_z, me_c = me_g // (2 * n_z), lax.rem(me_g // 2, n_z), lax.rem(me_g, 2)

    def for_grp_peers(act):
        n_x = n_grp // (2 * n_z)

        def row(step, last):
            half = (step + 1) // 2
            z = lax.rem(me_z + n_z // 2 + half * (1 - 2 * lax.rem(step, 2)) + n_z, n_z)
            for dx in sorted(range(n_x), key=lambda v: -min(v, n_x - v)):
                for dc in (1, 0):
                    if last and dx == 0 and dc == 0:
                        continue
                    x, c = lax.rem(me_x + dx, n_x), lax.rem(me_c + dc, 2)
                    act((x * n_z + z) * 2 + c)

        @pl.loop(0, n_z - 1)
        def _(step):
            row(step, False)

        row(jnp.int32(n_z - 1), True)

    def for_sub_peers(act):
        for d in sorted(range(1, n_sub), key=lambda v: -min(v, n_sub - v)):
            act(lax.rem(me_s + d, n_sub))

    def greet(g, s):
        pl.semaphore_signal(barrier, inc=1, device_id={"grp": g, "sub": s},
                            device_id_type=pl.DeviceIdType.MESH)

    for_grp_peers(lambda g: greet(g, me_s))
    for_sub_peers(lambda s: greet(me_g, s))
    loads[0].wait()
    flat = u_ref[...].reshape(ne * 8, ne).astype(F32)
    starts = range(0, ne, 128)
    for n, at in enumerate(starts):
        width = min(128, ne - at)
        uf[n, :, pl.ds(0, width)] = flat[:, at : at + width]
    loads[1].wait()
    loads[3].wait()
    total = jnp.zeros((ne, 128), F32)
    for c in range(8):
        tiles = [uf[n, pl.ds(c, ne, stride=8), :].astype(BF) for n in range(len(starts))]
        tiles[-1] = tiles[-1][:, : ne - starts[-1]]
        total += jnp.dot(jnp.concatenate(tiles, axis=1), x_ref[:, c * 128 : (c + 1) * 128],
                         preferred_element_type=F32)
    parent = total.astype(BF)
    twice = jnp.concatenate([p_ref[...], p_ref[...]], axis=0)
    packed = jnp.dot(twice, parent, preferred_element_type=F32).T.astype(BF).astype(F32)
    lo64 = lax.broadcasted_iota(I32, (1, 128), 1) < 64
    tab[pl.ds(0, 128), :] = packed
    tab[pl.ds(128, 8), :] = jnp.zeros((8, 128), F32)
    mine = jnp.where(lo64, packed[0:64], packed[64:128]).astype(BF)
    own[...] = mine
    ownr[me_s] = mine
    sf[...] = jnp.zeros_like(sf)
    loads[2].wait()

    @pl.loop(0, n_grp // 8)
    def _(step):
        for n in range(8):
            g = step * 8 + n
            for k in range(5):
                sf[g, pl.ds(k, 1), :] = jnp.where(lo64, tab[pl.ds(gs_ref[0, g * 10 + k], 1), :],
                                                  tab[pl.ds(gs_ref[0, g * 10 + 5 + k], 1), :])

    for j in range(3):
        send[:, j] = sf[:, 2 * j : 2 * j + 2, :].astype(BF)
    recv[me_g] = send[me_g]
    pl.semaphore_wait(barrier, n_grp + n_sub - 2)

    def own_copy(s):
        return pltpu.make_async_remote_copy(
            src_ref=own, dst_ref=ownr.at[me_s], send_sem=own_send, recv_sem=own_recv,
            device_id={"grp": me_g, "sub": s}, device_id_type=pl.DeviceIdType.MESH)

    def slot_copy(g):
        return pltpu.make_async_remote_copy(
            src_ref=send.at[g], dst_ref=recv.at[me_g], send_sem=slot_send, recv_sem=slot_recv,
            device_id={"grp": g, "sub": me_s}, device_id_type=pl.DeviceIdType.MESH)

    def gh_copy(s):
        return pltpu.make_async_remote_copy(
            src_ref=comp, dst_ref=ghr.at[me_s], send_sem=gh_send, recv_sem=gh_recv,
            device_id={"grp": me_g, "sub": s}, device_id_type=pl.DeviceIdType.MESH)

    for_grp_peers(lambda g: slot_copy(g).start())
    for_sub_peers(lambda s: own_copy(s).start())

    def iota(shape, dim):
        return lax.broadcasted_iota(I32, shape, dim)

    loads[4].wait()
    named = jnp.where(gv_ref[...] < 128, 1.0, 0.0)
    named = jnp.broadcast_to(named, (8, n_grp * 10)).astype(BF)
    slots = (n_grp * 10, 128)
    first = jnp.where(iota(slots, 0) == 10 * iota(slots, 1), 1.0, 0.0).astype(BF)
    near = jnp.dot(named, first, preferred_element_type=F32)
    square = (128, 128)
    below = jnp.where(iota(square, 0) < iota(square, 1), 1.0, 0.0).astype(BF)
    rank = jnp.dot(near.astype(BF), below, preferred_element_type=F32)
    ranks = rank.astype(I32)
    value = ((rank + 1.0) * near).astype(BF)
    wide = (128, n_grp * 8)
    copies = jnp.where(iota(wide, 0) == (iota(wide, 1) >> 3), 1.0, 0.0).astype(BF)
    value = jnp.dot(value, copies, preferred_element_type=F32)[0:1]
    k = iota((1, n_grp * 8), 1) & 7
    target = jnp.where((k < 5) & (value > 0.5), (value - 1.0) * 5.0 + k.astype(F32), -1.0)
    rows = iota((GH_ROWS, n_grp * 8), 0).astype(F32)
    hot[...] = jnp.where(rows == target, 1.0, 0.0).astype(BF)

    loads[5].wait()
    offs = nbr_ref.shape[0]
    tail = offs % 16
    idx_out[pl.ds(0, 8), :] = place(nbr_ref[pl.ds(0, 8), :], ranks)
    idx_out[pl.ds(8, 8), :] = jnp.concatenate(
        [place(nbr_ref[pl.ds(8, tail - 8), :], ranks), jnp.full((16 - tail, 128), ZERO_ROW, I32)], axis=0)
    for i in range((offs - tail) // 8):
        idx_out[pl.ds(8 * i + 16, 8), :] = place(nbr_ref[pl.ds(tail + 8 * i, 8), :], ranks)

    def all_slots(ref):
        return ref.at[pl.ds(0, n_grp - 1)]

    every_slot = pltpu.make_async_remote_copy(
        src_ref=all_slots(send), dst_ref=all_slots(recv), send_sem=slot_send, recv_sem=slot_recv,
        device_id={"grp": lax.rem(me_g + 1, n_grp), "sub": me_s}, device_id_type=pl.DeviceIdType.MESH)
    every_slot.wait_recv()
    for j in range(3):
        sf[:, 2 * j : 2 * j + 2, :] = recv[:, j].astype(F32)
    got = sf[...].reshape(n_grp * 8, 128).astype(BF)
    packed_ghosts = jnp.dot(hot[...], got, preferred_element_type=F32).astype(BF)
    comp[...] = packed_ghosts
    ghr[me_s] = packed_ghosts

    for_sub_peers(lambda s: gh_copy(s).start())

    def every(ref, src, s_sem, r_sem):
        part = ref.at[pl.ds(0, n_sub - 1)]
        return pltpu.make_async_remote_copy(
            src_ref=part, dst_ref=part, send_sem=s_sem, recv_sem=r_sem,
            device_id={"grp": me_g, "sub": lax.rem(me_s + 1, n_sub)}, device_id_type=pl.DeviceIdType.MESH)

    every_own = every(ownr, own, own_send, own_recv)
    every_own.wait_recv()
    own_out[...] = ownr[...]
    for h in range(4):
        turned = [ownr[s].astype(F32).T for s in (2 * h, 2 * h + 1)]
        own_flat[pl.ds(h * 64, 64), :] = jnp.concatenate(
            [t[at : at + 64] for t in turned for at in (0, 64)], axis=1).astype(BF)

    @pl.loop(0, idx_out.shape[0] // 16)
    def _(i):
        block = idx_out[pl.ds(pl.multiple_of(16 * i + 8, 8), 8), :]
        deep = iota((256, 256), 0)
        for o in range(0, 8, 2):
            v = jnp.concatenate([block[o : o + 1], block[o + 1 : o + 2]], axis=1)
            low, high = v & 255, v >> 8
            chosen = jnp.where(deep == low, 1.0, 0.0).astype(BF)
            each = jnp.dot(own_flat[...], chosen, preferred_element_type=F32)
            got = jnp.where(high == 0, each[0:64], 0.0)
            for h in range(1, 4):
                got = jnp.where(high == h, each[h * 64 : h * 64 + 64], got)
            part_out[i, :, pl.ds(o * 128, 256)] = got.astype(BF)

    every_slot.wait_send()
    every_own.wait_send()
    every_gh = every(ghr, comp, gh_send, gh_recv)
    every_gh.wait_recv()
    gh_out[...] = ghr[...]
    every_gh.wait_send()


def exchange(ghost_map, x, u, p, nbr, n_grp, n_sub):
    ne = u.shape[0]
    dma = pltpu.SemaphoreType.DMA
    return pl.pallas_call(
        functools.partial(exchange_kernel, n_grp, n_sub),
        out_shape=(
            jax.ShapeDtypeStruct((n_sub, 64, 128), BF),
            jax.ShapeDtypeStruct((n_sub, GH_ROWS, 128), BF),
            jax.ShapeDtypeStruct((320, 128), I32),
            jax.ShapeDtypeStruct((20, 64, 1024), BF),
        ),
        in_specs=[HB] * 5,
        out_specs=(VM, VM, VM, VM),
        scratch_shapes=[
            pltpu.SMEM(ghost_map.shape, I32),
            pltpu.VMEM(ghost_map.shape, I32),
            pltpu.VMEM(x.shape, BF),
            pltpu.VMEM(u.shape, BF),
            pltpu.VMEM(p.shape, BF),
            pltpu.VMEM(nbr.shape, I32),
            dma((6,)),
            pltpu.VMEM((pl.cdiv(ne, 128), ne * 8, 128), F32),
            pltpu.VMEM((136, 128), F32),
            pltpu.VMEM((n_grp, 8, 128), F32),
            pltpu.VMEM((n_grp, 3, 2, 128), BF),
            pltpu.VMEM((n_grp, 3, 2, 128), BF),
            pltpu.VMEM((64, 128), BF),
            pltpu.VMEM((n_sub, 64, 128), BF),
            pltpu.VMEM((GH_ROWS, 128), BF),
            pltpu.VMEM((n_sub, GH_ROWS, 128), BF),
            pltpu.VMEM((GH_ROWS, n_grp * 8), BF),
            pltpu.VMEM((256, 256), BF),
        ] + [dma] * 6,
        compiler_params=pltpu.CompilerParams(
            collective_id=0, has_side_effects=True, vmem_limit_bytes=24 * 2**20),
    )(*[pltpu.with_memory_space_constraint(a, pltpu.HBM) for a in (ghost_map, x, u, p, nbr)])

BUF = 3


def m2l_kernel(idx_ref, own_ref, gh_ref, part_ref, t_ref, e_hbm, d_hbm, out_ref,
               tab, flat, e_ref, d_ref, late_sem, sem, acc, dsc, *bufs):
    sms, sts = bufs[:BUF], bufs[BUF:]
    chunks = idx_ref.shape[0] // 16
    tiles = tab.shape[0] // 256 - 4
    e_load = pltpu.make_async_copy(e_hbm, e_ref, late_sem.at[0])
    d_load = pltpu.make_async_copy(d_hbm, d_ref, late_sem.at[1])
    e_load.start()
    d_load.start()

    def fetch(i, b):
        return pltpu.make_async_copy(idx_ref.at[pl.ds(pl.multiple_of(i * 16, 16), 8)], sms[b], sem.at[b])

    for b in range(BUF):
        fetch(b, b).start()
    lo64 = lax.broadcasted_iota(I32, (1, 128), 1) < 64

    def spread(src, base, rows):
        x = src.astype(F32)
        y = pltpu.roll(x, 64, 1)
        tab[pl.ds(base, rows), :] = jnp.where(lo64, x, y)
        tab[pl.ds(base + rows, rows), :] = jnp.where(lo64, y, x)

    for s in range(8):
        spread(own_ref[s], s * 128, 64)
        spread(gh_ref[s], 1024 + s * 2 * GH_ROWS, GH_ROWS)
    rest = tab.shape[0] - ZERO_ROW
    tab[pl.ds(ZERO_ROW, rest), :] = jnp.zeros((rest, 128), F32)
    for h in range(tiles):
        flat[pl.ds(h * 64, 64), :] = tab[pl.ds(1024 + h * 256, 256), :].T[:64].astype(BF)
    acc[...] = jnp.zeros_like(acc)

    def by_rows(sm, st, first):
        for o in range(0, 8, 2):
            for t in range(128):
                st[o // 2, pl.ds(t, 1), :] = jnp.where(
                    lo64, tab[pl.ds(sm[o, t], 1), :], tab[pl.ds(sm[o + 1, t], 1), :])
        p = jnp.concatenate([st[j] for j in range(4)], axis=1).astype(BF)
        return lax.dot_general(t_ref[:, pl.ds(pl.multiple_of(first * 64, 256), 512)], p, NT,
                               preferred_element_type=F32)

    def by_select(i, first, count):
        block = idx_ref[pl.ds(pl.multiple_of(16 * i + 8, 8), 8), :]
        deep = lax.broadcasted_iota(I32, (256, 256), 0)
        parts = []
        for o in range(0, count, 2):
            v = jnp.concatenate([block[o : o + 1], block[o + 1 : o + 2]], axis=1)
            low, high = v & 255, v >> 8
            hot = jnp.where(deep == low, 1.0, 0.0).astype(BF)
            every = jnp.dot(flat[...], hot, preferred_element_type=F32)
            got = part_ref[i, :, pl.ds(o * 128, 256)].astype(F32)
            for h in range(tiles):
                got = jnp.where(high == h + 4, every[h * 64 : h * 64 + 64], got)
            got = got.astype(BF)
            parts += [got[:, :128], got[:, 128:]]
        return jnp.dot(t_ref[:, pl.ds(pl.multiple_of(first * 64, 256), count * 64)],
                       jnp.concatenate(parts, axis=0), preferred_element_type=F32)

    def chunk(i, b, first, count=8):
        fetch(i, b).wait()
        acc[...] += by_rows(sms[b], sts[b], first) + by_select(i, first + 8, count)

    tail = t_ref.shape[1] // 64 - 16 * (chunks - 1)
    chunk(0, 0, 0, tail - 8)
    fetch(BUF, 0).start()
    chunk(1, 1, tail)
    fetch(BUF + 1, 1).start()

    @pl.loop(0, (chunks - 2) // BUF)
    def _(j):
        for c in range(BUF):
            b = (c + 2) % BUF
            i = BUF * j + c + 2
            chunk(i, b, tail + 16 * (i - 1))

            @pl.when(i + BUF < chunks)
            def _():
                fetch(i + BUF, b).start()

    lc = acc[...].astype(BF)
    e_load.wait()
    lm = lax.dot_general(e_ref[...], lc, (((0,), (0,)), ((), ())), preferred_element_type=F32).astype(BF)
    d_load.wait()
    ne = d_ref.shape[0]
    dsc[...] = jnp.dot(d_ref[...].reshape(ne * 8, ne), lm, preferred_element_type=F32)
    for c in range(8):
        out_ref[:, c * 128 : (c + 1) * 128] = dsc[pl.ds(c, ne, stride=8), :].astype(BF)


def m2l(idx, own, gh, part, t, e, d):
    ne = d.shape[0]
    table = pl.cdiv(ZERO_ROW + 1, 256) * 256
    return pl.pallas_call(
        m2l_kernel,
        out_shape=jax.ShapeDtypeStruct((ne, 1024), BF),
        in_specs=[VM] * 5 + [HB] * 2,
        out_specs=VM,
        scratch_shapes=[
            pltpu.VMEM((table, 128), F32),
            pltpu.VMEM((table // 4 - 256, 256), BF),
            pltpu.VMEM(e.shape[::-1], BF),
            pltpu.VMEM(d.shape, BF),
            pltpu.SemaphoreType.DMA((2,)),
            pltpu.SemaphoreType.DMA((BUF,)),
            pltpu.VMEM((64, 128), F32),
            pltpu.VMEM((ne * 8, 128), F32),
            *[pltpu.SMEM((8, 128), I32)] * BUF,
            *[pltpu.VMEM((4, 128, 128), F32)] * BUF,
        ],
        compiler_params=pltpu.CompilerParams(vmem_limit_bytes=24 * 2**20),
    )(idx, own, gh, part, t, *[pltpu.with_memory_space_constraint(a, pltpu.HBM) for a in (e.T, d)])


def on_device(
    child_moments,
    upward_matrix,
    project_matrix,
    transfer_matrix,
    expand_matrix,
    downward_matrix,
    neighbour_list,
    ghost_map,
):
    own, ghosts, index, part = exchange(ghost_map, child_moments, upward_matrix, project_matrix,
                                  neighbour_list, lax.axis_size("grp"), lax.axis_size("sub"))
    return m2l(index, own, ghosts, part, transfer_matrix, expand_matrix, downward_matrix)


def solution(mesh):
    return jax.shard_map(
        on_device,
        mesh=mesh,
        in_specs=(
            P(None, ("grp", "sub")),
            P(),
            P(),
            P(),
            P(),
            P(),
            P(None, ("grp", "sub")),
            P(("grp", "sub"), None),
        ),
        out_specs=P(None, ("grp", "sub")),
        check_vma=False,
    )
```
